256 devices in a mesh: parts: 2 (over z), row: 128 (over y, x, core).
Axes of the slice: x: 8, y: 8, z: 2, core: 2. Of those that a mesh axis runs over, the one named last changes fastest.
The devices are a block of a 8x8x16 slice.
Arguments:
- sigma_top: bfloat16 [4096, 2048], P(('parts', 'row')), parts along dimension 0, may hold values from -2 to 8, as said below
- panel_par: bfloat16 [4096, 1024], P(('parts', 'row')), parts along dimension 0, may hold values from -0.25 to 0.25
- dinv_par: float32 [2048, 1024], P(('parts', 'row')), parts along dimension 0, may hold values from -2 to 8, as said below
- panel_kid_top: bfloat16 [4, 2048, 1024], P('parts', 'row'), parts along dimension 0, may hold values from -0.25 to 0.25
- panel_kid_par: bfloat16 [4, 1024, 1024], P('parts', 'row'), parts along dimension 0, may hold values from -0.375 to 0.375
- dvar_kid: float32 [4, 1024], P('parts'), parts along dimension 0, may hold values from 0.5 to 2
- mask_par: int32 [16, 4], P('parts'), parts along dimension 0, may hold values 0 or 1
- mask_kid_top: int32 [4, 8, 4], P('parts'), parts along dimension 0, may hold values 0 or 1
- mask_kid_par: int32 [4, 4, 4], P('parts'), parts along dimension 0, may hold values 0 or 1
Outputs:
- cross_par: bfloat16 [4096, 1024], P(('parts', 'row')), parts along dimension 0
- sigma_par: bfloat16 [2048, 1024], P(('parts', 'row')), parts along dimension 0
- cross_kid_top: bfloat16 [4, 2048, 1024], P('parts', 'row'), parts along dimension 0
- cross_kid_par: bfloat16 [4, 1024, 1024], P('parts', 'row'), parts along dimension 0
- variance_kid: float32 [4, 1024], P('parts'), parts along dimension 0
The draws below stay inside these ranges and needn't reach their ends.
There are 2 independent parts, one for each index of `parts`. The reference program is written for one: setup_inputs(seed, part) draws one part's arguments, and reference() takes and returns one part's arrays. A program takes and returns all parts, laid end to end along the dimension named above; each array names one. Nothing has to cross between parts.
Inputs may be any that keep to these rules, and one draw needn't show every extreme that they name: `sigma_top`: symmetric positive definite. `dinv_par`: symmetric positive definite.
All inputs are finite; a program needn't handle non-finite values.
Results may differ from the reference program's by a relative error of at most 0.0052.
Values may be sent and summed in bfloat16 or wider, within the bound.
A program may use at most 64 MiB of HBM per device.

```python
import math
import jax
import jax.numpy as jnp
from jax import lax

WT = 2048
W1 = 1024
W2 = 1024
BLK = 256
KIDS = 2


def definite(key, width):
    first, second = jax.random.split(key, 2)
    raw = jax.random.normal(first, (width, width), jnp.float32)
    sym = (raw + raw.T) * (0.25 / jnp.sqrt(jnp.float32(width)))
    diag_part = jax.random.uniform(second, (width,), jnp.float32, 1.0, 2.0)
    whole = sym + jnp.diag(diag_part)
    return whole


def draw_sigma_top(key, part):
    return definite(jax.random.fold_in(key, 11), WT).astype(jnp.bfloat16)


def draw_dinv_par(key, part):
    return definite(jax.random.fold_in(key, 23), W1)


def place_ends(entries, key, low, high):
    longest = entries.shape.index(max(entries.shape))
    spots = []
    for shift in (0, 1):
        where = [jax.random.randint(jax.random.fold_in(key, axis), (), 0, length) for axis, length in enumerate(entries.shape)]
        where[longest] = (where[longest] + shift) % entries.shape[longest]
        spots.append(tuple(where))
    return entries.at[spots[0]].set(low).at[spots[1]].set(high)


def block_scale(rng, extent, shards, smallest, high):
    def one(position, parts):
        steps = jax.random.uniform(jax.random.fold_in(jax.random.fold_in(rng, 6), position), (parts,), jnp.float32, smallest / len(shards), high / len(shards))
        return jnp.repeat(jnp.exp(steps), extent[position] // parts).reshape((-1,) + (1,) * (len(extent) - position - 1))

    level = one(*shards[0])
    for cut in shards[1:]:
        level = level * one(*cut)
    return level


def noise(own_key, shape, spread, reach, cuts=(), dtype=jnp.bfloat16):
    entries = jax.random.normal(own_key, shape, jnp.float32) * spread
    if len(cuts) > 0:
        entries = block_scale(own_key, shape, cuts, -0.22, 0.18) * entries
    return jnp.clip(entries, min=-reach, max=reach).astype(dtype)


def setup_inputs(seed: int = 0, part: int = 0) -> dict:
    arg_keys = jax.random.split(jax.random.key(seed), 10)
    part_splits = jax.random.split(jax.random.fold_in(arg_keys[9], part), 10)
    return {
        "sigma_top": draw_sigma_top(jax.random.fold_in(jax.random.fold_in(arg_keys[9], part), 71), part),
        "panel_par": noise(part_splits[1], (WT, W1), (WT // 4) ** -0.5, 0.25, ((0, 128),)),
        "dinv_par": draw_dinv_par(jax.random.fold_in(jax.random.fold_in(arg_keys[9], part), 71), part),
        "panel_kid_top": noise(part_splits[3], (KIDS, WT, W2), (WT // 4) ** -0.5, 0.25, ((1, 128),)),
        "panel_kid_par": noise(part_splits[4], (KIDS, W1, W2), (W1 // 4) ** -0.5, 0.375, ((1, 128),)),
        "dvar_kid": jnp.clip(jnp.exp(jax.random.uniform(part_splits[5], (KIDS, W2), jnp.float32, math.log(0.5), math.log(2.0))), 0.5, 2.0),
        "mask_par": place_ends((jax.random.randint(part_splits[6], (WT // BLK, W1 // BLK), 0, 3) < 2).astype(jnp.int32), jax.random.fold_in(part_splits[6], 1), 0, 1),
        "mask_kid_top": place_ends((jax.random.randint(part_splits[7], (KIDS, WT // BLK, W2 // BLK), 0, 3) < 2).astype(jnp.int32), jax.random.fold_in(part_splits[7], 1), 0, 1),
        "mask_kid_par": place_ends((jax.random.randint(part_splits[8], (KIDS, W1 // BLK, W2 // BLK), 0, 3) < 2).astype(jnp.int32), jax.random.fold_in(part_splits[8], 1), 0, 1),
    }


def widen(mask):
    grown = jnp.repeat(jnp.repeat(mask, BLK, axis=-2), BLK, axis=-1)
    return grown.astype(jnp.bfloat16)


def reference(sigma_top, panel_par, dinv_par, panel_kid_top, panel_kid_par, dvar_kid, mask_par, mask_kid_top, mask_kid_par):
    high = lax.Precision.HIGHEST
    par_masked = panel_par * widen(mask_par)
    kid_top_masked = panel_kid_top * widen(mask_kid_top)
    kid_par_masked = panel_kid_par * widen(mask_kid_par)
    cross_par = jnp.dot(sigma_top, par_masked, preferred_element_type=jnp.float32).astype(jnp.bfloat16)
    sigma_par = (dinv_par + jnp.dot(par_masked.T, cross_par, preferred_element_type=jnp.float32)).astype(jnp.bfloat16)
    sig_wide = sigma_top.astype(jnp.float32)
    cross_wide = cross_par.astype(jnp.float32)
    spar_wide = sigma_par.astype(jnp.float32)
    ktop_wide = kid_top_masked.astype(jnp.float32)
    kpar_wide = kid_par_masked.astype(jnp.float32)
    kid_top = jnp.einsum("ac,kcw->kaw", sig_wide, ktop_wide, precision=high)
    kid_top = kid_top + jnp.einsum("ap,kpw->kaw", cross_wide, kpar_wide, precision=high)
    cross_kid_top = kid_top.astype(jnp.bfloat16)
    kid_par = jnp.einsum("ap,kaw->kpw", cross_wide, ktop_wide, precision=high)
    kid_par = kid_par + jnp.einsum("pq,kqw->kpw", spar_wide, kpar_wide, precision=high)
    cross_kid_par = kid_par.astype(jnp.bfloat16)
    variance_kid = dvar_kid + jnp.sum(ktop_wide * cross_kid_top.astype(jnp.float32), axis=1)
    variance_kid = variance_kid + jnp.sum(kpar_wide * cross_kid_par.astype(jnp.float32), axis=1)
    return cross_par, sigma_par, cross_kid_top, cross_kid_par, variance_kid
```

```python
import functools

import jax
import jax.numpy as jnp
from jax import lax
from jax.experimental import pallas as pl
from jax.experimental.pallas import tpu as pltpu
from jax.sharding import Mesh
from jax.sharding import PartitionSpec as P

BLK = 256
N = 8
T = 128
ROW = ("row_0", "row_1", "row_2")
PARTS_ROW = ("parts", "row_0", "row_1", "row_2")
BF = jnp.bfloat16
F32 = jnp.float32

(
    QX,
    PX,
    PD,
    KX,
    SX,
    SD,
    DX,
    DD,
    QY,
    CY,
    WY,
    YY,
    VY,
    CE,
    CD,
    CO,
    GY,
    GO,
    XO,
    YO,
    VO,
) = range(21)


def cols(i):
    return pl.ds(pl.multiple_of(i * T, T), T)


def dot(a, b):
    return jnp.dot(a, b, preferred_element_type=F32)


def kernel(
    sig,
    par,
    dinv,
    ktop,
    kpar,
    dvar,
    m_par,
    m_top,
    m_kpar,
    c_out,
    s_out,
    x_out,
    y_out,
    v_out,
    pm,
    km,
    qm,
    db,
    pr,
    pt,
    sr,
    dr,
    kb,
    qf,
    pc,
    wf,
    w32,
    yp,
    yr,
    dq,
    cp,
    cx,
    cb,
    gp,
    gr,
    gs,
    go,
    xb,
    yb,
    vp,
    vr,
    vs,
    vo,
    send,
    recv,
):
    y, x, c = (lax.axis_index(a) for a in ROW)
    o = 1 - c
    slot = x * 2 + c

    def at(yy, xx, cc):
        return {"row_0": yy, "row_1": xx, "row_2": cc}

    def put(phase, src, dst, where):
        pltpu.make_async_remote_copy(
            src_ref=src,
            dst_ref=dst,
            send_sem=send.at[phase],
            recv_sem=recv.at[phase],
            device_id=where,
            device_id_type=pl.DeviceIdType.MESH,
        ).start()

    def take(phase, ref):
        pltpu.make_async_copy(ref, ref, recv.at[phase]).wait()

    def flush(phase, ref):
        pltpu.make_async_copy(ref, ref, send.at[phase]).wait()

    def others(f):
        @pl.loop(1, N)
        def _(d):
            f(d)

    def along_x(f):
        others(lambda d: f(lax.rem(x + d, N)))

    def along_y(f):
        others(lambda d: f(lax.rem(y + d, N)))

    def row(f):
        @pl.loop(1, 2 * N)
        def _(d):
            s = lax.rem(slot + d, 2 * N)
            f(s, s // 2, lax.rem(s, 2))

    barrier = pltpu.get_barrier_semaphore()

    def greet(where):
        pl.semaphore_signal(
            barrier, inc=1, device_id=where, device_id_type=pl.DeviceIdType.MESH
        )

    row(lambda s, xx, cc: greet(at(y, xx, cc)))
    along_y(lambda yy: greet(at(yy, x, c)))

    per = ktop.shape[2] // m_top.shape[2]
    for j in range(m_kpar.shape[2]):
        s = pl.ds(j * per, per)
        for k in range(2):
            qm[k, :, s] = kpar[k, :, s] * m_kpar[k, y // 2, j].astype(F32).astype(BF)
            km[k, :, s] = ktop[k, :, s] * m_top[k, y, j].astype(F32).astype(BF)
        pm[:, s] = par[:, s] * m_par[y, j].astype(F32).astype(BF)
    db[...] = dinv[...].astype(BF)
    qf[y, slot] = qm[c, :, cols(x)]
    kb[slot] = km[c, :, cols(x)]
    pr[x, c] = pm[...]
    sr[x, c] = sig[...]
    dr[x, c] = db[...]
    pl.semaphore_wait(barrier, 2 * N - 1 + N - 1)

    row(lambda s, xx, cc: put(QX, qm.at[cc, :, cols(xx)], qf.at[y, slot], at(y, xx, cc)))
    along_x(lambda xx: put(PX, pm, pr.at[x, c], at(y, xx, c)))
    row(lambda s, xx, cc: put(KX, km.at[cc, :, cols(xx)], kb.at[slot], at(y, xx, cc)))
    along_x(lambda xx: put(SX, sig, sr.at[x, c], at(y, xx, c)))
    along_x(lambda xx: put(DX, db, dr.at[x, c], at(y, xx, c)))

    take(QX, qf.at[0, pl.ds(0, 2 * N - 1)])
    along_y(lambda yy: put(QY, qf.at[y], qf.at[y], at(yy, x, c)))

    take(PX, pr.at[pl.ds(0, N - 1), 0])
    put(PD, pr.at[:, c], pr.at[:, c], at(y, x, o))
    take(PD, pr.at[:, 0])
    half = pl.ds(c * (N // 2), N // 2)
    pc[y] = pr[half, :, :, cols(x)].reshape(T, T)
    along_y(lambda yy: put(CY, pc.at[y], pc.at[y], at(yy, x, c)))
    p_rows = pr[...].reshape(2 * T, N * T)
    for j in range(N):
        turned = p_rows[:, j * T : (j + 1) * T].T
        pt[j] = turned.reshape(N, 2, 8, 2 * T)

    take(KX, kb.at[pl.ds(0, 2 * N - 1)])
    take(QY, qf.at[pl.ds(0, N - 1)])
    q_all = qf[...].reshape(N * T, T)
    w = kb[...].reshape(2 * T, T).astype(F32) + dot(p_rows, q_all)
    w32[...] = w
    wf[y] = w.astype(BF)
    along_y(lambda yy: put(WY, wf.at[y], wf.at[y], at(yy, x, c)))

    take(SX, sr.at[pl.ds(0, N - 1), 0])
    put(SD, sr.at[:, c], sr.at[:, c], at(y, x, o))
    take(DX, dr.at[pl.ds(0, N - 1), 0])
    put(DD, dr.at[:, c], dr.at[:, c], at(y, x, o))
    take(DD, dr.at[:, 0])
    dq[...] = dot(dr[...].reshape(T, N * T), qf[...].reshape(N * T, T))
    take(SD, sr.at[:, 0])
    take(CY, pc.at[pl.ds(0, N - 1)])
    acc = jnp.zeros((2 * T, T), F32)
    for j in range(N):
        part = sr[:, :, :, pl.ds(pl.multiple_of((2 * j + c) * T, T), T)]
        acc = acc + dot(part.reshape(2 * T, T), pc[j])
    cp[...] = acc.reshape(2, T, T)
    put(CE, cp.at[o], cx, at(y, x, o))
    take(CE, cx)
    cb[half] = (cp[c] + cx[...]).astype(BF).reshape(N // 2, 2, 16, T)
    put(CD, cb.at[half], cb.at[half], at(y, x, o))
    take(CD, cb.at[pl.ds(0, N // 2)])
    along_x(lambda xx: put(CO, cb.at[xx, c], c_out.at[:, cols(x)], at(y, xx, c)))
    c_out[:, cols(x)] = cb[x, c]
    gp[...] = (
        dot(pt[:, :, c].reshape(N * T // 2, 2 * T), cb[...].reshape(2 * T, T))
        .astype(BF)
        .reshape(N, T // 2, T)
    )
    along_y(lambda yy: put(GY, gp.at[yy], gr.at[y], at(yy, x, c)))
    gr[y] = gp[y]

    take(WY, wf.at[pl.ds(0, N - 1)])
    xs = dot(sr[...].reshape(2 * T, 2 * N * T), wf[...].reshape(2 * N * T, T))
    xb[...] = xs.astype(BF).reshape(2 * N, 16, T)
    yp[...] = (
        dot(pt[...].reshape(N * T, 2 * T), xb[...].reshape(2 * T, T))
        .astype(BF)
        .reshape(N, T, T)
    )
    along_y(lambda yy: put(YY, yp.at[yy], yr.at[y], at(yy, x, c)))
    yr[y] = yp[y]
    q_own = qf[y].reshape(T, T).astype(F32)
    v = jnp.sum(w32[...] * xs, axis=0, keepdims=True)
    v = v + jnp.sum(q_own * dq[...], axis=0, keepdims=True)
    vp[...] = v
    vr[y] = v
    along_y(lambda yy: put(VY, vp, vr.at[y], at(yy, x, c)))
    row(lambda s, xx, cc: put(XO, xb.at[s], x_out.at[c, :, cols(x)], at(y, xx, cc)))
    x_out[c, :, cols(x)] = xb[slot]

    take(GY, gr.at[pl.ds(0, N - 1)])
    g = gr[0].astype(F32)
    for j in range(1, N):
        g = g + gr[j].astype(F32)
    gs[...] = g.reshape(N, 8, T)
    along_x(lambda xx: put(GO, gs.at[xx], go.at[x], at(y, xx, c)))
    go[x] = gs[x]

    take(YY, yr.at[pl.ds(0, N - 1)])
    yy_sum = dq[...]
    for j in range(N):
        yy_sum = yy_sum + yr[j].astype(F32)
    yb[...] = yy_sum.astype(BF).reshape(2 * N, 8, T)
    row(lambda s, xx, cc: put(YO, yb.at[s], y_out.at[c, :, cols(x)], at(y, xx, cc)))
    y_out[c, :, cols(x)] = yb[slot]
    take(VY, vr.at[pl.ds(0, N - 1)])
    v = jnp.sum(vr[...], axis=0)
    vs[...] = v
    vo[slot] = v
    row(lambda s, xx, cc: put(VO, vs, vo.at[slot], at(y, xx, cc)))

    take(GO, go.at[pl.ds(0, N - 1)])
    for j in range(N):
        s = pl.ds(j * T, T)
        s_out[:, s] = (dinv[:, s] + go[j]).astype(BF)
    take(VO, vo.at[pl.ds(0, 2 * N - 1)])
    for j in range(N):
        s = pl.ds(j * T, T)
        for k in range(2):
            v_out[pl.ds(k, 1), s] = dvar[pl.ds(k, 1), s] + vo[2 * j + k]
    take(CO, kb.at[pl.ds(0, N - 1)])
    take(XO, kb.at[pl.ds(0, 2 * N - 1)])
    take(YO, qf.at[0, pl.ds(0, 2 * N - 1)])

    flush(QX, qf.at[0, pl.ds(0, 2 * N - 1)])
    flush(PX, pr.at[pl.ds(0, N - 1), 0])
    flush(PD, pr.at[:, 0])
    flush(KX, kb.at[pl.ds(0, 2 * N - 1)])
    flush(SX, sr.at[pl.ds(0, N - 1), 0])
    flush(SD, sr.at[:, 0])
    flush(DX, dr.at[pl.ds(0, N - 1), 0])
    flush(DD, dr.at[:, 0])
    flush(QY, qf.at[pl.ds(0, N - 1)])
    flush(CY, pc.at[pl.ds(0, N - 1)])
    flush(WY, wf.at[pl.ds(0, N - 1)])
    flush(YY, yr.at[pl.ds(0, N - 1)])
    flush(VY, vr.at[pl.ds(0, N - 1)])
    flush(CE, cx)
    flush(CD, cb.at[pl.ds(0, N // 2)])
    flush(CO, kb.at[pl.ds(0, N - 1)])
    flush(GY, gr.at[pl.ds(0, N - 1)])
    flush(GO, go.at[pl.ds(0, N - 1)])
    flush(XO, kb.at[pl.ds(0, 2 * N - 1)])
    flush(YO, qf.at[0, pl.ds(0, 2 * N - 1)])
    flush(VO, vo.at[pl.ds(0, 2 * N - 1)])


def shards(sig, par, dinv, ktop, kpar, dvar, m_par, m_top, m_kpar):
    vmem = pl.BlockSpec(memory_space=pltpu.VMEM)
    smem = pl.BlockSpec(memory_space=pltpu.SMEM)
    like = jax.ShapeDtypeStruct
    V = pltpu.VMEM
    return pl.pallas_call(
        kernel,
        name="selected_inverse",
        out_shape=(
            like(par.shape, BF),
            like(dinv.shape, BF),
            like(ktop.shape, BF),
            like(kpar.shape, BF),
            like(dvar.shape, F32),
        ),
        in_specs=[vmem] * 6 + [smem] * 3,
        out_specs=(vmem,) * 5,
        scratch_shapes=[
            V(par.shape, BF),
            V(ktop.shape, BF),
            V(kpar.shape, BF),
            V(dinv.shape, BF),
            V((N, 2, *par.shape), BF),
            V((N, N, 2, 8, 2 * T), BF),
            V((N, 2, *sig.shape), BF),
            V((N, 2, *dinv.shape), BF),
            V((2 * N, 16, T), BF),
            V((N, 2 * N, 8, T), BF),
            V((N, T, T), BF),
            V((N, 2 * T, T), BF),
            V((2 * T, T), F32),
            V((N, T, T), BF),
            V((N, T, T), BF),
            V((T, T), F32),
            V((2, T, T), F32),
            V((T, T), F32),
            V((N, 2, 16, T), BF),
            V((N, T // 2, T), BF),
            V((N, T // 2, T), BF),
            V((N, 8, T), F32),
            V((N, 8, T), F32),
            V((2 * N, 16, T), BF),
            V((2 * N, 8, T), BF),
            V((1, T), F32),
            V((N, 1, T), F32),
            V((1, T), F32),
            V((2 * N, 1, T), F32),
            pltpu.SemaphoreType.DMA((21,)),
            pltpu.SemaphoreType.DMA((21,)),
        ],
        compiler_params=pltpu.CompilerParams(collective_id=0, has_side_effects=True),
    )(sig, par, dinv, ktop, kpar, dvar, m_par, m_top, m_kpar)


def solution(mesh):
    finer = Mesh(
        mesh.devices.reshape(mesh.shape["parts"], N, N, 2), ("parts", "row_0", "row_1", "row_2")
    )
    return jax.shard_map(
        shards,
        mesh=finer,
        in_specs=(
            P(PARTS_ROW, None),
            P(PARTS_ROW, None),
            P(PARTS_ROW, None),
            P("parts", ROW, None),
            P("parts", ROW, None),
            P("parts", None),
            P("parts", None),
            P("parts", None, None),
            P("parts", None, None),
        ),
        out_specs=(
            P(PARTS_ROW, None),
            P(PARTS_ROW, None),
            P("parts", ROW, None),
            P("parts", ROW, None),
            P("parts", None),
        ),
        check_vma=False,
    )
```
